64 devices in a mesh: sys: 4 (over x, y), seg: 16 (over z, core).
Axes of the slice: x: 2, y: 2, z: 8, core: 2. Of those that a mesh axis runs over, the one named last changes fastest.
The devices are a block of a 4x4x8 slice.
Arguments:
- positions: bfloat16 [196608, 320], P(('sys', 'seg')), parts along dimension 0
- charges: float32 [196608], P(('sys', 'seg')), parts along dimension 0
- pair_band: int32 [64, 15], P(('sys', 'seg')), parts along dimension 0
Outputs:
- output 1: float32 [196608, 320], P(('sys', 'seg')), parts along dimension 0
- output 2: float32 [4], P('sys'), parts along dimension 0
There are 4 independent parts. The reference program is written for one: setup_inputs(seed, part) draws one part's arguments, and reference() takes and returns one part's arrays. A program takes and returns all parts, laid end to end along the dimension named above; each array names one.
All inputs are finite; a program needn't handle non-finite values.
Results may differ from the reference program's by a relative error of at most 0.001.
Values are sent between devices in bfloat16 or wider.
A program may use at most 768 MiB of HBM per device.

```python
import jax
import jax.numpy as jnp
from jax import lax

SEG_COUNT = 16
BLOCK_ROWS = 3072
FEAT_DIM = 320
REACH_STEPS = 7


def draw_band(mask_key):
    coin_draw = jax.random.randint(mask_key, (SEG_COUNT, REACH_STEPS), 0, 3)
    block_ids = jnp.arange(SEG_COUNT)[:, None]
    step_ids = jnp.arange(REACH_STEPS)[None, :]
    upper_cols = jnp.where((block_ids == 0) & (step_ids == REACH_STEPS - 1), 1, (coin_draw > 0).astype(jnp.int32))
    lower_list = [jnp.roll(upper_cols[:, step_idx - 1], step_idx) for step_idx in range(REACH_STEPS, 0, -1)]
    higher_list = [upper_cols[:, step_idx - 1] for step_idx in range(1, REACH_STEPS + 1)]
    centre_list = [jnp.ones((SEG_COUNT,), jnp.int32)]
    return jnp.stack(lower_list + centre_list + higher_list, axis=1).astype(jnp.int32)


def setup_inputs(seed: int = 0, part: int = 0) -> dict:
    part_key = jax.random.fold_in(jax.random.key(seed), part)
    pos_key, sign_key, mag_key, mask_key = jax.random.split(part_key, 4)
    all_rows = SEG_COUNT * BLOCK_ROWS
    pos_vals = jax.random.normal(pos_key, (all_rows, FEAT_DIM), jnp.float32)
    sign_vals = 2.0 * jax.random.randint(sign_key, (all_rows,), 0, 2).astype(jnp.float32) - 1.0
    magnitude = jax.random.uniform(mag_key, (all_rows,), jnp.float32, 0.5, 1.5)
    charge_scale = FEAT_DIM ** 0.5 * (BLOCK_ROWS * (2 * REACH_STEPS + 1)) ** -0.25
    return {'positions': pos_vals.astype(jnp.bfloat16), 'charges': sign_vals * magnitude * charge_scale, 'pair_band': draw_band(mask_key)}


def reference(positions, charges, pair_band):
    inv_lsq = 1.0 / FEAT_DIM
    pos_blocks = positions.reshape(SEG_COUNT, BLOCK_ROWS, FEAT_DIM)
    charge_blocks = charges.reshape(SEG_COUNT, BLOCK_ROWS)
    row_ids = jnp.arange(BLOCK_ROWS)
    self_pair = row_ids[:, None] == row_ids[None, :]
    offsets = jnp.arange(-REACH_STEPS, REACH_STEPS + 1)

    def one_block(host_blk):
        x_host = pos_blocks[host_blk]
        host_f32 = x_host.astype(jnp.float32)
        host_sq = jnp.sum(host_f32 * host_f32, axis=1)
        q_host = charge_blocks[host_blk]

        def one_offset(carry_state, offset):
            force_acc, energy_acc = carry_state
            other_blk = (host_blk + offset) % SEG_COUNT
            x_other = pos_blocks[other_blk]
            other_f32 = x_other.astype(jnp.float32)
            other_sq = jnp.sum(other_f32 * other_f32, axis=1)
            cross_dot = jnp.dot(x_host, x_other.T, preferred_element_type=jnp.float32)
            sq_dist = jnp.maximum(host_sq[:, None] + other_sq[None, :] - 2.0 * cross_dot, 0.0)
            weights = q_host[:, None] * charge_blocks[other_blk][None, :] * jnp.exp(sq_dist * (-0.5 * inv_lsq))
            keep_pair = (pair_band[host_blk, REACH_STEPS + offset] != 0) & jnp.logical_not(self_pair & (offset == 0))
            weights = jnp.where(keep_pair, weights, 0.0)
            pull_term = jnp.dot(weights.astype(jnp.bfloat16), x_other, preferred_element_type=jnp.float32)
            force_acc = force_acc + (jnp.sum(weights, axis=1)[:, None] * host_f32 - pull_term) * inv_lsq
            energy_acc = energy_acc + 0.5 * jnp.sum(weights)
            return (force_acc, energy_acc), None

        init_carry = (jnp.zeros((BLOCK_ROWS, FEAT_DIM), jnp.float32), jnp.zeros((), jnp.float32))
        (force_blk, energy_blk), _ = lax.scan(one_offset, init_carry, offsets)
        return force_blk, energy_blk

    force_blocks, block_energy = lax.map(one_block, jnp.arange(SEG_COUNT))
    return force_blocks.reshape(SEG_COUNT * BLOCK_ROWS, FEAT_DIM), jnp.sum(block_energy).reshape(1)
```

```python
import functools
import math

import jax
import jax.numpy as jnp
from jax import lax
from jax.experimental import pallas as pl
from jax.experimental.pallas import tpu as pltpu
from jax.sharding import PartitionSpec as P

CHUNKS = (768, 768, 768, 768)
LOCAL_CHUNK = 768
I_TILE = 512
EXTRA = 16
TERMS = 3


def split_terms(values):
    high = lax.reduce_precision(values, 8, 7)
    rest = values - high
    mid = lax.reduce_precision(rest, 8, 7)
    low = rest - mid
    return [piece.astype(jnp.bfloat16) for piece in (high, mid, low)]


def pair_kernel(feat, n_blocks, masked, vis_width, meta_ref, *refs):
    if masked:
        own_ref, partner_ref = refs[:2]
        refs = refs[2:]
    else:
        vis_ref = refs[0]
        refs = refs[1:]
    host_ref, charge_ref, sel_ref, acc_in, sum_in, acc_ref, sum_ref, vis_buf, vis_rows, vis_charge, sems = refs
    packed = feat + EXTRA
    depth = vis_buf.shape[1]
    n_host = host_ref.shape[2]
    count = meta_ref[0]
    scale = -math.log2(math.e) * 0.5 / feat
    acc_ref[...] = acc_in[...]
    sum_ref[...] = sum_in[...]
    vis_buf[:, packed:, :] = jnp.zeros((2, depth - packed, vis_width), jnp.bfloat16)

    def fetch(step, slot, wait):
        dst = vis_buf.at[slot, pl.ds(0, packed), :]
        if masked:
            cols = pl.ds(pl.multiple_of(lax.rem(step, n_blocks) * vis_width, 128), vis_width)
            if wait:
                pltpu.make_async_copy(own_ref.at[:, cols], dst, sems.at[slot]).wait()
            else:
                @pl.when(step < n_blocks)
                def _():
                    pltpu.make_async_copy(own_ref.at[:, cols], dst, sems.at[slot]).start()

                @pl.when(step >= n_blocks)
                def _():
                    pltpu.make_async_copy(partner_ref.at[:, cols], dst, sems.at[slot]).start()
        else:
            copy = pltpu.make_async_copy(vis_ref.at[meta_ref[2 + step]], dst, sems.at[slot])
            copy.wait() if wait else copy.start()

    n_list = 2 * n_blocks if masked else n_blocks

    @pl.when(count > 0)
    def _():
        fetch(0, 0, False)

    def one_visitor(step, carry):
        slot = lax.rem(step, 2)
        fetch(step, slot, True)

        @pl.when(step + 1 < count)
        def _():
            fetch(step + 1, 1 - slot, False)

        vis_rows[...] = vis_buf[slot].T
        vis_charge[...] = jnp.dot(vis_rows[:, depth - 128:], sel_ref[...], preferred_element_type=jnp.float32)
        vis_t = vis_buf.at[slot, pl.ds(0, feat), :]

        for host in range(2):
            @pl.when(meta_ref[2 + n_list * (1 + host) + step] != 0)
            def _():
                for tile in range(n_host // I_TILE):
                    cols = slice(tile * I_TILE, (tile + 1) * I_TILE)
                    near = jnp.dot(vis_rows[...], host_ref[host, :, cols], preferred_element_type=jnp.float32)
                    decay = jnp.exp2(jnp.maximum(near, 0.0) * scale)
                    charge_j = jnp.concatenate([vis_charge[...]] * (I_TILE // 128), axis=1)
                    weights = decay * charge_ref[host, :, cols] * charge_j
                    if masked:
                        row = lax.broadcasted_iota(jnp.int32, weights.shape, 0)
                        col = lax.broadcasted_iota(jnp.int32, weights.shape, 1)
                        gap = meta_ref[1] + tile * I_TILE - lax.rem(step, n_blocks) * vis_width
                        gap = jnp.where((step >= n_blocks) == (host == 1), gap, -(2 ** 20))
                        weights = jnp.where(row - col == gap, 0.0, weights)
                    sum_ref[host, :, cols] += jnp.sum(weights.reshape(vis_width // 8, 8, I_TILE), axis=0)
                    acc_ref[host, :, cols] += jnp.dot(vis_t[...], weights.astype(jnp.bfloat16), preferred_element_type=jnp.float32)
        return carry

    lax.fori_loop(0, count, one_visitor, 0)


def solution(mesh):
    seg_len = mesh.shape['seg']
    swap = [(dev, dev ^ 1) for dev in range(seg_len)]

    def device_fn(positions, charges, pair_band):
        n_rows, feat = positions.shape
        reach = (pair_band.shape[1] - 1) // 2
        half = n_rows // 2
        packed = feat + EXTRA
        depth = -(-packed // 128) * 128
        me = lax.axis_index('seg')
        core = lax.rem(me, 2)
        first = core * half

        xf = positions.astype(jnp.float32)
        square = jnp.minimum(jnp.sum(xf * xf, axis=1), 3.0e38)
        neg_sq = split_terms(-square)
        ones = jnp.ones((TERMS, n_rows), jnp.bfloat16)
        pad = jnp.zeros((EXTRA - 3 * TERMS, n_rows), jnp.bfloat16)
        own = jnp.concatenate([positions.T, jnp.stack([-p for p in neg_sq]), ones, jnp.stack(split_terms(charges)), pad], axis=0)

        gathered = []
        start = 0
        for width in CHUNKS:
            gathered.append(lax.all_gather(own[:, start:start + width], 'seg'))
            start += width
        partner = lax.ppermute(own, 'seg', swap)
        partner_band = lax.ppermute(pair_band[0], 'seg', swap)

        hosts = jnp.stack([lax.dynamic_slice(own, (0, first), (packed, half)), lax.dynamic_slice(partner, (0, first), (packed, half))])
        host_t = jnp.concatenate([
            -2 * hosts[:, :feat],
            jnp.ones((2, TERMS, half), jnp.bfloat16),
            hosts[:, feat:feat + TERMS],
            jnp.zeros((2, depth - feat - 2 * TERMS, half), jnp.bfloat16)], axis=1)
        host_q = jnp.sum(hosts[:, feat + 2 * TERMS:feat + 3 * TERMS].astype(jnp.float32), axis=1, keepdims=True)
        sel_row = jnp.arange(128) - (feat + 2 * TERMS - (depth - 128))
        select = jnp.broadcast_to(((sel_row >= 0) & (sel_row < TERMS))[:, None], (128, 128)).astype(jnp.bfloat16)

        others = jnp.arange(seg_len)

        def live_of(block, band):
            step = jnp.mod(others - block + seg_len // 2, seg_len) - seg_len // 2
            inside = jnp.abs(step) <= reach
            return inside & (jnp.sum(jnp.where(jnp.arange(2 * reach + 1)[None, :] == (step + reach)[:, None], band[None, :], 0), axis=1) != 0)

        own_live = live_of(me, pair_band[0])
        partner_live = live_of(me ^ 1, partner_band)
        far = (others // 2) != (me // 2)
        any_live = (own_live | partner_live) & far
        place = jnp.sum(any_live[None, :] & (others[None, :] < others[:, None]), axis=1)
        pick = any_live[None, :] & (place[None, :] == others[:, None])

        def in_order(values):
            return jnp.sum(jnp.where(pick, values[None, :], 0), axis=1)

        far_meta = jnp.concatenate([
            jnp.stack([jnp.sum(any_live), first]), in_order(others),
            in_order(own_live.astype(jnp.int32)), in_order(partner_live.astype(jnp.int32))]).astype(jnp.int32)
        n_local = n_rows // LOCAL_CHUNK
        near_live = jnp.where(core == 0, pair_band[0, reach + 1], pair_band[0, reach - 1])
        link_flags = jnp.full((n_local,), near_live)
        yes = jnp.ones((n_local,), jnp.int32)
        near_meta = jnp.concatenate([
            jnp.stack([2 * n_local, first]), jnp.zeros((2 * n_local,), jnp.int32),
            yes, link_flags, link_flags, yes]).astype(jnp.int32)

        any_space = pl.BlockSpec(memory_space=pl.ANY)
        vmem = pl.BlockSpec(memory_space=pltpu.VMEM)
        smem = pl.BlockSpec(memory_space=pltpu.SMEM)

        def call(masked, width, n_blocks, meta, visitors, acc, sums):
            n_vis = len(visitors)
            return pl.pallas_call(
                functools.partial(pair_kernel, feat, n_blocks, masked, width),
                out_shape=[jax.ShapeDtypeStruct(acc.shape, acc.dtype), jax.ShapeDtypeStruct(sums.shape, sums.dtype)],
                in_specs=[smem] + [any_space] * n_vis + [vmem] * 5,
                out_specs=[vmem, vmem],
                scratch_shapes=[
                    pltpu.VMEM((2, depth, width), jnp.bfloat16),
                    pltpu.VMEM((width, depth), jnp.bfloat16),
                    pltpu.VMEM((width, 128), jnp.float32),
                    pltpu.SemaphoreType.DMA((2,)),
                ],
                input_output_aliases={n_vis + 4: 0, n_vis + 5: 1},
                compiler_params=pltpu.CompilerParams(vmem_limit_bytes=56 * 2 ** 20),
                cost_estimate=pl.CostEstimate(flops=2 * 8 * n_rows * width * feat * 2, bytes_accessed=2 ** 23, transcendentals=n_rows * width * 8),
                name='near_pairs' if masked else 'far_pairs',
            )(meta, *visitors, host_t, host_q, select, acc, sums)

        acc = jnp.zeros((2, feat, half), jnp.float32)
        sums = jnp.zeros((2, 8, half), jnp.float32)
        acc, sums = call(True, LOCAL_CHUNK, n_local, near_meta, [own, partner], acc, sums)
        for width, block in zip(CHUNKS, gathered):
            acc, sums = call(False, width, seg_len, far_meta, [block], acc, sums)

        totals = jnp.sum(sums, axis=1)
        energy = lax.psum(0.5 * jnp.sum(totals), 'seg')
        pulled = (totals[:, None, :] * hosts[:, :feat].astype(jnp.float32) - acc) * (1.0 / feat)
        pulled = jnp.swapaxes(pulled, 1, 2)
        other = lax.ppermute(pulled[1], 'seg', swap)
        forces = jnp.where(core == 0, jnp.concatenate([pulled[0], other]), jnp.concatenate([other, pulled[0]]))
        return forces, energy.reshape(1)

    row_spec = P(('sys', 'seg'), None)
    vec_spec = P(('sys', 'seg'))
    return jax.shard_map(device_fn, mesh=mesh, in_specs=(row_spec, vec_spec, row_spec), out_specs=(row_spec, P('sys')), check_vma=False)
```

```python
import functools
import math

import jax
import jax.numpy as jnp
from jax import lax
from jax.experimental import pallas as pl
from jax.experimental.pallas import tpu as pltpu
from jax.sharding import PartitionSpec as P

CHUNKS = 4
TILE = 256
EXTRA = 16
DEPTH = 384
MESH = pl.DeviceIdType.MESH

SQUARE, ONES, CHARGE, HOST_CHARGE = 0, 3, 6, 9


def pieces(values):
    high = values.astype(jnp.bfloat16).astype(jnp.float32)
    rest = values - high
    mid = rest.astype(jnp.bfloat16).astype(jnp.float32)
    return [high, mid, rest - mid]


def pack_kernel(x_ref, q_ref, *out_refs):
    feat, n_rows = x_ref.shape
    width = n_rows // CHUNKS
    for chunk in range(CHUNKS):
        cols = slice(chunk * width, (chunk + 1) * width)
        x = x_ref[:, cols]
        xf = x.astype(jnp.float32)
        square = jnp.minimum(jnp.sum(xf * xf, axis=0, keepdims=True), 3.0e38)
        ones = jnp.ones((3, width), jnp.float32)
        extra = jnp.concatenate(pieces(square) + [ones] + pieces(q_ref[:, cols]) + [jnp.zeros((EXTRA - 9, width), jnp.float32)], axis=0)
        extra = extra.astype(jnp.bfloat16)
        for ref in (out_refs[chunk], out_refs[CHUNKS].at[chunk]):
            ref[:feat, :] = x
            ref[feat:, :] = extra


def pair_task(vis_ref, host, gap, keep, host_ref, charge_ref, acc_ref, sum_ref):
    feat, half = acc_ref.shape[1:]
    width = vis_ref.shape[1]
    scale = -math.log2(math.e) * 0.5 / feat
    extra = vis_ref[feat:feat + EXTRA, :].astype(jnp.float32)
    charge_j = extra[CHARGE:CHARGE + 1] + extra[CHARGE + 1:CHARGE + 2] + extra[CHARGE + 2:CHARGE + 3]
    if keep is not None:
        charge_j = jnp.where(keep, charge_j, 0.0)

    def span(tile):
        return slice(tile * TILE, (tile + 1) * TILE)

    def distance(tile):
        return jnp.dot(host_ref[host, span(tile), :], vis_ref[...], preferred_element_type=jnp.float32)

    ahead = distance(0)
    for tile in range(half // TILE):
        near = ahead
        if (tile + 1) * TILE < half:
            ahead = distance(tile + 1)
        charge_i = jnp.concatenate([charge_ref[host, span(tile), :]] * (width // 128), axis=1)
        weights = jnp.exp2(jnp.maximum(near, 0.0) * scale) * charge_i * charge_j
        if gap is not None:
            row = lax.broadcasted_iota(jnp.int32, weights.shape, 0)
            col = lax.broadcasted_iota(jnp.int32, weights.shape, 1)
            weights = jnp.where(col - row == gap + tile * TILE, 0.0, weights)
        part = weights[:, :128]
        for group in range(1, width // 128):
            part = part + weights[:, group * 128:(group + 1) * 128]
        sum_ref[host, span(tile), :] += part
        acc_ref[host, :, span(tile)] += lax.dot_general(
            vis_ref[:feat, :], weights.astype(jnp.bfloat16), (((1,), (1,)), ((), ())), preferred_element_type=jnp.float32)


def host_charges(host_ref, charge_ref, feat):
    base = DEPTH - 128
    row = lax.broadcasted_iota(jnp.int32, (128, 128), 0) + base - feat - HOST_CHARGE
    pick = jnp.where((row >= 0) & (row < 3), 1.0, 0.0).astype(jnp.bfloat16)
    for host in range(2):
        charge_ref[host] = jnp.dot(host_ref[host, :, base:], pick, preferred_element_type=jnp.float32)


def near_kernel(seg_len, reach, band_ref, own_ref, partner_ref, list_ref, host_ref, acc_ref, sum_ref, vis, charges, sems):
    feat = own_ref.shape[1] - EXTRA
    width = own_ref.shape[2]
    half = CHUNKS * width // 2
    per_half = CHUNKS // 2
    me = lax.axis_index('seg')
    core = lax.rem(me, 2)
    copies = []
    for side, ref in enumerate((own_ref, partner_ref)):
        for chunk in range(CHUNKS):
            slot = side * CHUNKS + chunk
            copies.append(pltpu.make_async_copy(ref.at[chunk], vis.at[slot, pl.ds(0, feat + EXTRA), :], sems.at[slot]))
            copies[-1].start()
    vis[:, feat + EXTRA:, :] = jnp.zeros((2 * CHUNKS, DEPTH - feat - EXTRA, width), jnp.bfloat16)
    acc_ref[...] = jnp.zeros_like(acc_ref)
    sum_ref[...] = jnp.zeros_like(sum_ref)

    n_list = 2 * seg_len
    list_ref[0] = 0

    def clear(i, carry):
        list_ref[i] = 0
        return carry

    lax.fori_loop(0, list_ref.shape[0], clear, 0)
    for host in range(2):
        block = me if host == 0 else me + 1 - 2 * core

        def add(other, count):
            step = lax.rem(other - block + seg_len + seg_len // 2, seg_len) - seg_len // 2
            inside = (step >= -reach) & (step <= reach) & (other // 2 != me // 2)
            live = inside & (band_ref[host, jnp.clip(step + reach, 0, 2 * reach)] != 0)

            @pl.when(live)
            def _():
                list_ref[1 + count] = other
                list_ref[1 + n_list + 2 + count] = host

            return count + live.astype(jnp.int32)

        list_ref[0] = lax.fori_loop(0, seg_len, add, list_ref[0])

    for copy in copies:
        copy.wait()
    for host in range(2):
        for part in range(per_half):
            slot = host * CHUNKS + core * per_half + part
            block = vis[slot]
            extra = block[feat:feat + EXTRA].astype(jnp.float32)
            width_zero = jnp.zeros((3, width), jnp.float32)
            extra = jnp.concatenate([
                extra[ONES:ONES + 3], extra[SQUARE:SQUARE + 3], width_zero, extra[CHARGE:CHARGE + 3],
                jnp.zeros((EXTRA - 12, width), jnp.float32)], axis=0).astype(jnp.bfloat16)
            full = jnp.concatenate([-2 * block[:feat], extra, jnp.zeros((DEPTH - feat - EXTRA, width), jnp.bfloat16)], axis=0)
            host_ref[host, part * width:(part + 1) * width, :] = full.T
    host_charges(host_ref, charges, feat)

    def run(slot, host, gap):
        pair_task(vis.at[slot], host, gap, None, host_ref, charges, acc_ref, sum_ref)

    def masked(step, carry):
        host = step // per_half
        part = lax.rem(step, per_half)
        run(host * CHUNKS + core * per_half + part, host, -part * width)
        return carry

    def unmasked(step, carry):
        far_step = step - 2
        host = jnp.where(step < 2, step, far_step // per_half)
        base = jnp.where(step < 2, step * CHUNKS + (1 - core) * per_half, (1 - host) * CHUNKS + lax.rem(step, 2) * per_half)
        for part in range(per_half):
            run(base + part, host, None)
        return carry

    lax.fori_loop(0, CHUNKS, masked, 0)
    linked = band_ref[0, reach + 1 - 2 * core] != 0
    lax.fori_loop(0, jnp.where(linked, 2 + CHUNKS, 2), unmasked, 0)


def far_kernel(list_ref, vis_ref, host_ref, acc_old, sum_old, acc_ref, sum_ref, vis, charges, acc_prev, sum_prev, sems, old_sems):
    feat = acc_ref.shape[1]
    width = vis.shape[3]
    n_list = (list_ref.shape[0] - 1) // 2
    count = list_ref[0]
    old = [pltpu.make_async_copy(acc_old, acc_prev, old_sems.at[0]), pltpu.make_async_copy(sum_old, sum_prev, old_sems.at[1])]

    def fetch(pair, slot):
        return [pltpu.make_async_copy(
            vis_ref.at[list_ref[1 + 2 * pair + u]], vis.at[slot, u, pl.ds(0, feat + EXTRA), :], sems.at[slot, u]) for u in range(2)]

    for copy in fetch(0, 0) + old:
        copy.start()
    vis[:, :, feat + EXTRA:, :] = jnp.zeros((2, 2, DEPTH - feat - EXTRA, width), jnp.bfloat16)
    acc_ref[...] = jnp.zeros_like(acc_ref)
    sum_ref[...] = jnp.zeros_like(sum_ref)
    host_charges(host_ref, charges, feat)

    def run(slot, u, task):
        pair_task(vis.at[slot, u], list_ref[1 + n_list + task], None, (task < count) if u else None, host_ref, charges, acc_ref, sum_ref)

    def two_tasks(pair, carry):
        slot = lax.rem(pair, 2)
        for copy in fetch(pair, slot):
            copy.wait()
        for copy in fetch(pair + 1, 1 - slot):
            copy.start()
        for u in range(2):
            run(slot, u, 2 * pair + u)
        return carry

    pairs = (count + 1) // 2
    lax.fori_loop(0, pairs, two_tasks, 0)
    for copy in fetch(pairs, lax.rem(pairs, 2)):
        copy.wait()

    for copy in old:
        copy.wait()
    acc_ref[...] += acc_prev[...]
    sum_ref[...] += sum_prev[...]


def total_kernel(n, x_ref, out_ref, slots, send_sems, recv_sems):
    me = lax.axis_index('seg')
    barrier = pltpu.get_barrier_semaphore()
    for k in range(1, n):
        pl.semaphore_signal(barrier, inc=1, device_id={'seg': lax.rem(me + k, n)}, device_id_type=MESH)
    pl.semaphore_wait(barrier, n - 1)
    sends = []
    for k in range(1, n):
        sends.append(pltpu.make_async_remote_copy(
            src_ref=x_ref, dst_ref=slots.at[me], send_sem=send_sems.at[k], recv_sem=recv_sems.at[me],
            device_id={'seg': lax.rem(me + k, n)}, device_id_type=MESH))
        sends[-1].start()
    slots[me] = x_ref[...]
    for k in range(1, n):
        owner = lax.rem(me + k, n)
        pltpu.make_async_remote_copy(
            src_ref=x_ref, dst_ref=slots.at[owner], send_sem=send_sems.at[k], recv_sem=recv_sems.at[owner],
            device_id={'seg': owner}, device_id_type=MESH).wait_recv()
    for send in sends:
        send.wait_send()
    total = slots[0]
    for k in range(1, n):
        total = total + slots[k]
    out_ref[...] = total


def solution(mesh):
    seg_len = mesh.shape['seg']
    swap = [(dev, dev ^ 1) for dev in range(seg_len)]
    any_space = pl.BlockSpec(memory_space=pl.ANY)
    vmem = pl.BlockSpec(memory_space=pltpu.VMEM)
    smem = pl.BlockSpec(memory_space=pltpu.SMEM)

    def device_fn(positions, charges, pair_band):
        n_rows, feat = positions.shape
        reach = (pair_band.shape[1] - 1) // 2
        half = n_rows // 2
        width = n_rows // CHUNKS
        core = lax.rem(lax.axis_index('seg'), 2)
        shape = jax.ShapeDtypeStruct
        big = pltpu.CompilerParams(vmem_limit_bytes=60 * 2 ** 20)
        packed = (feat + EXTRA, width)

        x_t = positions.T
        *parts, own = pl.pallas_call(
            pack_kernel,
            out_shape=[shape(packed, jnp.bfloat16)] * CHUNKS + [shape((CHUNKS,) + packed, jnp.bfloat16)],
            in_specs=[vmem, vmem],
            out_specs=[vmem] * (CHUNKS + 1),
            compiler_params=big,
            name='pack',
        )(x_t, charges[None, :])
        gathered = [lax.all_gather(part, 'seg') for part in parts]
        partner = lax.ppermute(own, 'seg', swap)
        bands = jnp.concatenate([pair_band, lax.ppermute(pair_band, 'seg', swap)])

        acc_shape = shape((2, feat, half), jnp.float32)
        sum_shape = shape((2, half, 128), jnp.float32)
        host_shape = shape((2, half, DEPTH), jnp.bfloat16)
        n_list = 2 * seg_len + 2
        pair_flops = 4 * half * width * DEPTH
        tasks, host, acc, sums = pl.pallas_call(
            functools.partial(near_kernel, seg_len, reach),
            out_shape=[shape((1 + 2 * n_list,), jnp.int32), host_shape, acc_shape, sum_shape],
            in_specs=[smem, any_space, any_space],
            out_specs=[smem, vmem, vmem, vmem],
            scratch_shapes=[
                pltpu.VMEM((2 * CHUNKS, DEPTH, width), jnp.bfloat16),
                pltpu.VMEM((2, half, 128), jnp.float32),
                pltpu.SemaphoreType.DMA((2 * CHUNKS,)),
            ],
            compiler_params=big,
            cost_estimate=pl.CostEstimate(flops=16 * pair_flops, bytes_accessed=2 ** 24, transcendentals=16 * half * width),
            name='near_pairs',
        )(bands, own, partner)
        for block in gathered:
            acc, sums = pl.pallas_call(
                far_kernel,
                out_shape=[acc_shape, sum_shape],
                in_specs=[smem, any_space, vmem, any_space, any_space],
                out_specs=[vmem, vmem],
                scratch_shapes=[
                    pltpu.VMEM((2, 2, DEPTH, width), jnp.bfloat16),
                    pltpu.VMEM((2, half, 128), jnp.float32),
                    pltpu.VMEM(acc_shape.shape, jnp.float32),
                    pltpu.VMEM(sum_shape.shape, jnp.float32),
                    pltpu.SemaphoreType.DMA((2, 2)),
                    pltpu.SemaphoreType.DMA((2,)),
                ],
                compiler_params=big,
                cost_estimate=pl.CostEstimate(flops=20 * pair_flops, bytes_accessed=2 ** 25, transcendentals=20 * half * width),
                name='far_pairs',
            )(tasks, block, host, acc, sums)

        totals = jnp.sum(sums, axis=2)
        energy_part = jnp.sum(totals.reshape(-1, 8, 128), axis=0)
        energy_all = pl.pallas_call(
            functools.partial(total_kernel, seg_len),
            out_shape=shape((8, 128), jnp.float32),
            in_specs=[vmem],
            out_specs=vmem,
            scratch_shapes=[
                pltpu.VMEM((seg_len, 8, 128), jnp.float32),
                pltpu.SemaphoreType.DMA((seg_len,)),
                pltpu.SemaphoreType.DMA((seg_len,)),
            ],
            compiler_params=pltpu.CompilerParams(collective_id=0, has_side_effects=True),
            name='energy_total',
        )(energy_part)
        energy = 0.5 * jnp.sum(energy_all)

        first = core * half
        x_own = lax.dynamic_slice(x_t, (0, first), (feat, half)).astype(jnp.float32)
        partner_x = jnp.concatenate([lax.dynamic_index_in_dim(partner, core * (CHUNKS // 2) + part, 0, False)[:feat] for part in range(CHUNKS // 2)], axis=1)
        force_own = (totals[0][None, :] * x_own - acc[0]) * (1.0 / feat)
        force_partner = (totals[1][None, :] * partner_x.astype(jnp.float32) - acc[1]) * (1.0 / feat)
        other = lax.ppermute(force_partner, 'seg', swap)
        forces = jnp.where(core == 0, jnp.concatenate([force_own, other], axis=1), jnp.concatenate([other, force_own], axis=1))
        return forces.T, energy.reshape(1)

    row_spec = P(('sys', 'seg'), None)
    vec_spec = P(('sys', 'seg'))
    return jax.shard_map(device_fn, mesh=mesh, in_specs=(row_spec, vec_spec, row_spec), out_specs=(row_spec, P('sys')), check_vma=False)
```

```python
import functools
import math

import jax
import jax.numpy as jnp
from jax import lax
from jax.experimental import pallas as pl
from jax.experimental.pallas import tpu as pltpu
from jax.sharding import PartitionSpec as P

CHUNKS = 6
TILE = 256
EXTRA = 8
DEPTH = 384
MESH = pl.DeviceIdType.MESH

SQUARE, CHARGE, HOST_CHARGE = 0, 3, 11


def pieces(values):
    high = values.astype(jnp.bfloat16).astype(jnp.float32)
    rest = values - high
    mid = rest.astype(jnp.bfloat16).astype(jnp.float32)
    return [high, mid, rest - mid]


def pack_kernel(chunks, x_ref, q_ref, *out_refs):
    feat = x_ref.shape[0]
    width = out_refs[0].shape[-1]
    for chunk in chunks:
        cols = slice(chunk * width, (chunk + 1) * width)
        x = x_ref[:, cols]
        xf = x.astype(jnp.float32)
        square = jnp.minimum(jnp.sum(xf * xf, axis=0, keepdims=True), 3.0e38)
        extra = jnp.concatenate(pieces(square) + pieces(q_ref[:, cols]) + [jnp.zeros((EXTRA - 6, width), jnp.float32)], axis=0)
        extra = extra.astype(jnp.bfloat16)
        targets = out_refs if len(chunks) == 1 else [out_refs[-1].at[chunk]] + ([out_refs[chunk - 1]] if chunk else [])
        for ref in targets:
            ref[:feat, :] = x
            ref[feat:, :] = extra


def lower_rows(feat, width):
    n_low = DEPTH - feat - EXTRA
    row = lax.broadcasted_iota(jnp.int32, (n_low, width), 0)
    return jnp.where(row < 3, 1.0, 0.0).astype(jnp.bfloat16)


def pair_task(vis_ref, host, gap, keep, host_ref, charge_ref, acc_ref, sum_ref):
    feat, half = acc_ref.shape[1:]
    width = vis_ref.shape[1]
    scale = -math.log2(math.e) * 0.5 / feat
    extra = vis_ref[feat:feat + EXTRA, :].astype(jnp.float32)
    charge_j = extra[CHARGE:CHARGE + 1] + extra[CHARGE + 1:CHARGE + 2] + extra[CHARGE + 2:CHARGE + 3]
    if keep is not None:
        charge_j = jnp.where(keep, charge_j, 0.0)

    def span(tile):
        return slice(tile * TILE, (tile + 1) * TILE)

    def distance(tile):
        return jnp.dot(host_ref[host, span(tile), :], vis_ref[...], preferred_element_type=jnp.float32)

    def pull(weights, tile):
        acc_ref[host, :, span(tile)] += lax.dot_general(
            vis_ref[:feat, :], weights, (((1,), (1,)), ((), ())), preferred_element_type=jnp.float32)

    n_tiles = half // TILE
    ahead = distance(0)
    behind = None
    for tile in range(n_tiles):
        charge_i = jnp.concatenate([charge_ref[host, span(tile), :]] * (width // 128), axis=1)
        weights = jnp.exp2(jnp.maximum(ahead, 0.0) * scale) * charge_i * charge_j
        if gap is not None:
            row = lax.broadcasted_iota(jnp.int32, weights.shape, 0)
            col = lax.broadcasted_iota(jnp.int32, weights.shape, 1)
            weights = jnp.where(col - row == gap + tile * TILE, 0.0, weights)
        part = weights[:, :128]
        for group in range(1, width // 128):
            part = part + weights[:, group * 128:(group + 1) * 128]
        sum_ref[host, span(tile), :] += part
        if tile + 1 < n_tiles:
            ahead = distance(tile + 1)
        if behind is not None:
            pull(behind, tile - 1)
        behind = weights.astype(jnp.bfloat16)
    pull(behind, n_tiles - 1)


def sweep(acc_ref, sum_ref, step):
    for number, ref, rows in ((0, acc_ref, 8), (1, sum_ref, 96)):
        def one(k, carry):
            step(number, (slice(None), pl.ds(pl.multiple_of(k * rows, 8), rows), slice(None)))
            return carry

        lax.fori_loop(0, ref.shape[1] // rows, one, 0)


def clear_sums(acc_ref, sum_ref):
    refs = (acc_ref, sum_ref)

    def step(number, rows):
        refs[number][rows] = jnp.zeros_like(refs[number][rows])

    sweep(acc_ref, sum_ref, step)


def host_charges(host_ref, charge_ref, feat):
    base = DEPTH - 128
    row = lax.broadcasted_iota(jnp.int32, (128, 128), 0) + base - feat - HOST_CHARGE
    pick = jnp.where((row >= 0) & (row < 3), 1.0, 0.0).astype(jnp.bfloat16)
    for host in range(2):
        charge_ref[host] = jnp.dot(host_ref[host, :, base:], pick, preferred_element_type=jnp.float32)


def near_kernel(seg_len, reach, band_ref, own_ref, partner_ref, list_ref, host_ref, acc_ref, sum_ref, vis, charges, sems):
    feat = own_ref.shape[1] - EXTRA
    width = own_ref.shape[2]
    half = CHUNKS * width // 2
    per_half = CHUNKS // 2
    me = lax.axis_index('seg')
    core = lax.rem(me, 2)
    copies = []
    for side, ref in enumerate((own_ref, partner_ref)):
        for chunk in range(CHUNKS):
            slot = side * CHUNKS + chunk
            copies.append(pltpu.make_async_copy(ref.at[chunk], vis.at[slot, pl.ds(0, feat + EXTRA), :], sems.at[slot]))
            copies[-1].start()
    low = lower_rows(feat, width)
    for slot in range(2 * CHUNKS):
        vis[slot, feat + EXTRA:, :] = low
    clear_sums(acc_ref, sum_ref)

    n_list = 2 * seg_len
    list_ref[0] = 0

    def clear(i, carry):
        list_ref[i] = 0
        return carry

    lax.fori_loop(0, list_ref.shape[0], clear, 0)
    for host in range(2):
        block = me if host == 0 else me + 1 - 2 * core

        def add(other, count):
            step = lax.rem(other - block + seg_len + seg_len // 2, seg_len) - seg_len // 2
            inside = (step >= -reach) & (step <= reach) & (other // 2 != me // 2)
            live = inside & (band_ref[host, jnp.clip(step + reach, 0, 2 * reach)] != 0)

            @pl.when(live)
            def _():
                list_ref[1 + count] = other
                list_ref[1 + n_list + 2 + count] = host

            return count + live.astype(jnp.int32)

        list_ref[0] = lax.fori_loop(0, seg_len, add, list_ref[0])

    for copy in copies:
        copy.wait()
    for host in range(2):
        for part in range(per_half):
            slot = host * CHUNKS + core * per_half + part
            block = vis[slot]
            extra = block[feat:feat + EXTRA].astype(jnp.float32)
            n_low = DEPTH - feat - EXTRA
            upper = jnp.concatenate([jnp.ones((3, width), jnp.float32), jnp.zeros((EXTRA - 3, width), jnp.float32)], axis=0)
            lower = jnp.concatenate([
                extra[SQUARE:SQUARE + 3], extra[CHARGE:CHARGE + 3], jnp.zeros((n_low - 6, width), jnp.float32)], axis=0)
            below = jnp.concatenate([upper, lower], axis=0).astype(jnp.bfloat16)
            full = jnp.concatenate([-2 * block[:feat], below], axis=0)
            host_ref[host, part * width:(part + 1) * width, :] = full.T
    host_charges(host_ref, charges, feat)

    def run(slot, host, gap):
        pair_task(vis.at[slot], host, gap, None, host_ref, charges, acc_ref, sum_ref)

    def masked(step, carry):
        host = step // per_half
        part = lax.rem(step, per_half)
        run(host * CHUNKS + core * per_half + part, host, -part * width)
        return carry

    def unmasked(step, carry):
        far_step = step - CHUNKS
        host = jnp.where(step < CHUNKS, step // per_half, far_step // CHUNKS)
        base = jnp.where(step < CHUNKS, host * CHUNKS + (1 - core) * per_half + lax.rem(step, per_half), (1 - host) * CHUNKS + lax.rem(step, CHUNKS))
        run(base, host, None)
        return carry

    lax.fori_loop(0, CHUNKS, masked, 0)
    linked = band_ref[0, reach + 1 - 2 * core] != 0
    lax.fori_loop(0, jnp.where(linked, 3 * CHUNKS, CHUNKS), unmasked, 0)


def far_kernel(last, list_ref, vis_ref, host_ref, acc_old, sum_old, *refs):
    if last:
        own_ref, partner_ref, acc_ref, energy_ref, vis, charges, acc_prev, sum_prev, sems, old_sems, sum_ref, x_buf, x_sems = refs
    else:
        acc_ref, sum_ref, vis, charges, acc_prev, sum_prev, sems, old_sems = refs
    feat = acc_ref.shape[1]
    width = vis.shape[3]
    n_list = (list_ref.shape[0] - 1) // 2
    count = list_ref[0]
    old = [pltpu.make_async_copy(acc_old, acc_prev, old_sems.at[0]), pltpu.make_async_copy(sum_old, sum_prev, old_sems.at[1])]

    def fetch(pair, slot):
        return [pltpu.make_async_copy(
            vis_ref.at[list_ref[1 + 2 * pair + u]], vis.at[slot, u, pl.ds(0, feat + EXTRA), :], sems.at[slot, u]) for u in range(2)]

    if last:
        per_half = acc_ref.shape[2] // width
        core = lax.rem(lax.axis_index('seg'), 2)
        for host, ref in enumerate((own_ref, partner_ref)):
            for part in range(per_half):
                old.append(pltpu.make_async_copy(
                    ref.at[core * per_half + part, pl.ds(0, feat), :], x_buf.at[host, :, pl.ds(part * width, width)], x_sems.at[host, part]))
    for copy in fetch(0, 0) + old:
        copy.start()
    low = lower_rows(feat, width)
    for slot in range(2):
        for u in range(2):
            vis[slot, u, feat + EXTRA:, :] = low
    clear_sums(acc_ref, sum_ref)
    host_charges(host_ref, charges, feat)

    def run(slot, u, task):
        pair_task(vis.at[slot, u], list_ref[1 + n_list + task], None, (task < count) if u else None, host_ref, charges, acc_ref, sum_ref)

    def two_tasks(pair, carry):
        slot = lax.rem(pair, 2)
        for copy in fetch(pair, slot):
            copy.wait()
        for copy in fetch(pair + 1, 1 - slot):
            copy.start()
        for u in range(2):
            run(slot, u, 2 * pair + u)
        return carry

    pairs = (count + 1) // 2
    lax.fori_loop(0, pairs, two_tasks, 0)
    for copy in fetch(pairs, lax.rem(pairs, 2)):
        copy.wait()

    for copy in old:
        copy.wait()
    if not last:
        def step(number, rows):
            (acc_ref, sum_ref)[number][rows] += (acc_prev, sum_prev)[number][rows]

        sweep(acc_ref, sum_ref, step)
        return
    half = acc_ref.shape[2]
    energy = jnp.zeros((8, 128), jnp.float32)
    for host in range(2):
        sums = sum_ref[host] + sum_prev[host]
        energy = energy + jnp.sum(sums.reshape(half // 8, 8, 128), axis=0)
        total = jnp.zeros((8, half), jnp.float32)
        for piece in pieces(sums):
            total = total + lax.dot_general(
                jnp.ones((8, 128), jnp.bfloat16), piece.astype(jnp.bfloat16), (((1,), (1,)), ((), ())), preferred_element_type=jnp.float32)
        pulled = acc_ref[host] + acc_prev[host]
        acc_ref[host] = (total[0:1] * x_buf[host].astype(jnp.float32) - pulled) * (1.0 / feat)
    energy_ref[...] = energy


def join_kernel(mine_ref, other_ref, out_ref, bounce, sems):
    half = other_ref.shape[1]
    core = lax.rem(lax.axis_index('seg'), 2)
    sources = [mine_ref.at[0], other_ref]
    loads = [pltpu.make_async_copy(sources[k], bounce.at[k], sems.at[0, k]) for k in range(2)]
    for load in loads:
        load.start()
    stores = []
    for k in range(2):
        place = pl.multiple_of((core if k == 0 else 1 - core) * half, 128)
        loads[k].wait()
        stores.append(pltpu.make_async_copy(bounce.at[k], out_ref.at[:, pl.ds(place, half)], sems.at[1, k]))
        stores[-1].start()
    for store in stores:
        store.wait()


def total_kernel(n, x_ref, out_ref, slots, send_sems, recv_sems):
    me = lax.axis_index('seg')
    barrier = pltpu.get_barrier_semaphore()
    for k in range(1, n):
        pl.semaphore_signal(barrier, inc=1, device_id={'seg': lax.rem(me + k, n)}, device_id_type=MESH)
    pl.semaphore_wait(barrier, n - 1)
    sends = []
    for k in range(1, n):
        sends.append(pltpu.make_async_remote_copy(
            src_ref=x_ref, dst_ref=slots.at[me], send_sem=send_sems.at[k], recv_sem=recv_sems.at[me],
            device_id={'seg': lax.rem(me + k, n)}, device_id_type=MESH))
        sends[-1].start()
    slots[me] = x_ref[...]
    for k in range(1, n):
        owner = lax.rem(me + k, n)
        pltpu.make_async_remote_copy(
            src_ref=x_ref, dst_ref=slots.at[owner], send_sem=send_sems.at[k], recv_sem=recv_sems.at[owner],
            device_id={'seg': owner}, device_id_type=MESH).wait_recv()
    for send in sends:
        send.wait_send()
    total = slots[0]
    for k in range(1, n):
        total = total + slots[k]
    out_ref[...] = total


def solution(mesh):
    seg_len = mesh.shape['seg']
    swap = [(dev, dev ^ 1) for dev in range(seg_len)]
    any_space = pl.BlockSpec(memory_space=pl.ANY)
    vmem = pl.BlockSpec(memory_space=pltpu.VMEM)
    smem = pl.BlockSpec(memory_space=pltpu.SMEM)

    def device_fn(positions, charges, pair_band):
        n_rows, feat = positions.shape
        reach = (pair_band.shape[1] - 1) // 2
        half = n_rows // 2
        width = n_rows // CHUNKS
        shape = jax.ShapeDtypeStruct
        big = pltpu.CompilerParams(vmem_limit_bytes=60 * 2 ** 20)
        packed = (feat + EXTRA, width)

        x_t = positions.T
        charge_row = charges[None, :]
        first_part = pl.pallas_call(
            functools.partial(pack_kernel, (0,)),
            grid=(1,),
            out_shape=shape(packed, jnp.bfloat16),
            in_specs=[pl.BlockSpec((feat, width), lambda i: (0, 0)), pl.BlockSpec((1, width), lambda i: (0, 0))],
            out_specs=pl.BlockSpec(packed, lambda i: (0, 0)),
            name='pack_first',
        )(x_t, charge_row)
        *parts, own = pl.pallas_call(
            functools.partial(pack_kernel, tuple(range(CHUNKS))),
            out_shape=[shape(packed, jnp.bfloat16)] * (CHUNKS - 1) + [shape((CHUNKS,) + packed, jnp.bfloat16)],
            in_specs=[vmem, vmem],
            out_specs=[vmem] * CHUNKS,
            compiler_params=big,
            name='pack',
        )(x_t, charge_row)
        parts = [first_part] + parts
        gathered = [lax.all_gather(part, 'seg') for part in parts]
        partner = lax.ppermute(own, 'seg', swap)
        bands = jnp.concatenate([pair_band, lax.ppermute(pair_band, 'seg', swap)])

        acc_shape = shape((2, feat, half), jnp.float32)
        sum_shape = shape((2, half, 128), jnp.float32)
        host_shape = shape((2, half, DEPTH), jnp.bfloat16)
        n_list = 2 * seg_len + 2
        pair_flops = 4 * half * width * DEPTH
        tasks, host, acc, sums = pl.pallas_call(
            functools.partial(near_kernel, seg_len, reach),
            out_shape=[shape((1 + 2 * n_list,), jnp.int32), host_shape, acc_shape, sum_shape],
            in_specs=[smem, any_space, any_space],
            out_specs=[smem, vmem, vmem, vmem],
            scratch_shapes=[
                pltpu.VMEM((2 * CHUNKS, DEPTH, width), jnp.bfloat16),
                pltpu.VMEM((2, half, 128), jnp.float32),
                pltpu.SemaphoreType.DMA((2 * CHUNKS,)),
            ],
            compiler_params=big,
            cost_estimate=pl.CostEstimate(flops=16 * pair_flops, bytes_accessed=2 ** 24, transcendentals=16 * half * width),
            name='near_pairs',
        )(bands, own, partner)
        for chunk, block in enumerate(gathered):
            last = chunk == CHUNKS - 1
            scratch = [
                pltpu.VMEM((2, 2, DEPTH, width), jnp.bfloat16),
                pltpu.VMEM((2, half, 128), jnp.float32),
                pltpu.VMEM(acc_shape.shape, jnp.float32),
                pltpu.VMEM(sum_shape.shape, jnp.float32),
                pltpu.SemaphoreType.DMA((2, 2)),
                pltpu.SemaphoreType.DMA((2,)),
            ]
            if last:
                scratch += [
                    pltpu.VMEM(sum_shape.shape, jnp.float32),
                    pltpu.VMEM(acc_shape.shape, jnp.bfloat16),
                    pltpu.SemaphoreType.DMA((2, CHUNKS // 2)),
                ]
            acc, sums = pl.pallas_call(
                functools.partial(far_kernel, last),
                out_shape=[acc_shape, shape((8, 128), jnp.float32) if last else sum_shape],
                in_specs=[smem, any_space, vmem, any_space, any_space] + [any_space] * (2 if last else 0),
                out_specs=[vmem, vmem],
                scratch_shapes=scratch,
                compiler_params=big,
                cost_estimate=pl.CostEstimate(flops=20 * pair_flops, bytes_accessed=2 ** 25, transcendentals=20 * half * width),
                name='last_pairs' if last else 'far_pairs',
            )(tasks, block, host, acc, sums, *((own, partner) if last else ()))

        other = lax.ppermute(acc[1], 'seg', swap)
        energy_all = pl.pallas_call(
            functools.partial(total_kernel, seg_len),
            out_shape=shape((8, 128), jnp.float32),
            in_specs=[vmem],
            out_specs=vmem,
            scratch_shapes=[
                pltpu.VMEM((seg_len, 8, 128), jnp.float32),
                pltpu.SemaphoreType.DMA((seg_len,)),
                pltpu.SemaphoreType.DMA((seg_len,)),
            ],
            compiler_params=pltpu.CompilerParams(collective_id=0, has_side_effects=True),
            name='energy_total',
        )(sums)
        energy = 0.5 * jnp.sum(energy_all)

        forces = pl.pallas_call(
            join_kernel,
            out_shape=shape((feat, n_rows), jnp.float32),
            in_specs=[any_space, any_space],
            out_specs=any_space,
            scratch_shapes=[pltpu.VMEM((2, feat, half), jnp.float32), pltpu.SemaphoreType.DMA((2, 2))],
            name='join_halves',
        )(acc, other)
        return forces.T, energy.reshape(1)

    row_spec = P(('sys', 'seg'), None)
    vec_spec = P(('sys', 'seg'))
    return jax.shard_map(device_fn, mesh=mesh, in_specs=(row_spec, vec_spec, row_spec), out_specs=(row_spec, P('sys')), check_vma=False)
```

```python
import functools
import math

import jax
import jax.numpy as jnp
from jax import lax
from jax.experimental import pallas as pl
from jax.experimental.pallas import tpu as pltpu
from jax.sharding import PartitionSpec as P

CHUNKS = 4
TILE = 256
EXTRA = 8
DEPTH = 384
MESH = pl.DeviceIdType.MESH

SQUARE, CHARGE, HOST_CHARGE = 0, 3, 11


def pieces(values):
    high = values.astype(jnp.bfloat16).astype(jnp.float32)
    rest = values - high
    mid = rest.astype(jnp.bfloat16).astype(jnp.float32)
    return [high, mid, rest - mid]


def pack_kernel(chunks, x_ref, q_ref, *out_refs):
    feat = x_ref.shape[0]
    width = out_refs[0].shape[-1]
    for chunk in chunks:
        cols = slice(chunk * width, (chunk + 1) * width)
        x = x_ref[:, cols]
        xf = x.astype(jnp.float32)
        square = jnp.minimum(jnp.sum(xf * xf, axis=0, keepdims=True), 3.0e38)
        extra = jnp.concatenate(pieces(square) + pieces(q_ref[:, cols]) + [jnp.zeros((EXTRA - 6, width), jnp.float32)], axis=0)
        extra = extra.astype(jnp.bfloat16)
        targets = out_refs if len(chunks) == 1 else [out_refs[-1].at[chunk]] + ([out_refs[chunk - 1]] if chunk else [])
        for ref in targets:
            ref[:feat, :] = x
            ref[feat:, :] = extra


def lower_rows(feat, width):
    n_low = DEPTH - feat - EXTRA
    row = lax.broadcasted_iota(jnp.int32, (n_low, width), 0)
    return jnp.where(row < 3, 1.0, 0.0).astype(jnp.bfloat16)


def pair_task(vis_ref, host, gap, keep, host_ref, charge_ref, acc_ref, sum_ref):
    feat, half = acc_ref.shape[1:]
    width = vis_ref.shape[1]
    scale = -math.log2(math.e) * 0.5 / feat
    extra = vis_ref[feat:feat + EXTRA, :].astype(jnp.float32)
    charge_j = extra[CHARGE:CHARGE + 1] + extra[CHARGE + 1:CHARGE + 2] + extra[CHARGE + 2:CHARGE + 3]
    if keep is not None:
        charge_j = jnp.where(keep, charge_j, 0.0)

    def span(tile):
        return slice(tile * TILE, (tile + 1) * TILE)

    def distance(tile):
        return jnp.dot(host_ref[host, span(tile), :], vis_ref[...], preferred_element_type=jnp.float32)

    def pull(weights, tile):
        acc_ref[host, :, span(tile)] += lax.dot_general(
            vis_ref[:feat, :], weights, (((1,), (1,)), ((), ())), preferred_element_type=jnp.float32)

    n_tiles = half // TILE
    ahead = distance(0)
    behind = None
    for tile in range(n_tiles):
        charge_i = jnp.concatenate([charge_ref[host, span(tile), :]] * (width // 128), axis=1)
        weights = jnp.exp2(jnp.maximum(ahead, 0.0) * scale) * charge_i * charge_j
        if gap is not None:
            row = lax.broadcasted_iota(jnp.int32, weights.shape, 0)
            col = lax.broadcasted_iota(jnp.int32, weights.shape, 1)
            weights = jnp.where(col - row == gap + tile * TILE, 0.0, weights)
        part = weights[:, :128]
        for group in range(1, width // 128):
            part = part + weights[:, group * 128:(group + 1) * 128]
        sum_ref[host, span(tile), :] += part
        if tile + 1 < n_tiles:
            ahead = distance(tile + 1)
        if behind is not None:
            pull(behind, tile - 1)
        behind = weights.astype(jnp.bfloat16)
    pull(behind, n_tiles - 1)


def sweep(acc_ref, sum_ref, step):
    for number, ref, rows in ((0, acc_ref, 64), (1, sum_ref, 512)):
        def one(k, carry):
            step(number, (slice(None), pl.ds(pl.multiple_of(k * rows, 8), rows), slice(None)))
            return carry

        lax.fori_loop(0, ref.shape[1] // rows, one, 0)


def clear_sums(acc_ref, sum_ref):
    refs = (acc_ref, sum_ref)

    def step(number, rows):
        refs[number][rows] = jnp.zeros_like(refs[number][rows])

    sweep(acc_ref, sum_ref, step)


def host_charges(host_ref, charge_ref, feat):
    base = DEPTH - 128
    row = lax.broadcasted_iota(jnp.int32, (128, 128), 0) + base - feat - HOST_CHARGE
    pick = jnp.where((row >= 0) & (row < 3), 1.0, 0.0).astype(jnp.bfloat16)
    for host in range(2):
        charge_ref[host] = jnp.dot(host_ref[host, :, base:], pick, preferred_element_type=jnp.float32)


def near_kernel(seg_len, reach, band_ref, own_ref, partner_ref, list_ref, host_ref, acc_ref, sum_ref, vis, charges, sems):
    feat = own_ref.shape[1] - EXTRA
    width = own_ref.shape[2]
    half = CHUNKS * width // 2
    per_half = CHUNKS // 2
    me = lax.axis_index('seg')
    core = lax.rem(me, 2)
    copies = []
    for side, ref in enumerate((own_ref, partner_ref)):
        for chunk in range(CHUNKS):
            slot = side * CHUNKS + chunk
            copies.append(pltpu.make_async_copy(ref.at[chunk], vis.at[slot, pl.ds(0, feat + EXTRA), :], sems.at[slot]))
            copies[-1].start()
    low = lower_rows(feat, width)
    for slot in range(2 * CHUNKS):
        vis[slot, feat + EXTRA:, :] = low
    clear_sums(acc_ref, sum_ref)

    n_list = 2 * seg_len
    list_ref[0] = 0

    def clear(i, carry):
        list_ref[i] = 0
        return carry

    lax.fori_loop(0, list_ref.shape[0], clear, 0)
    for host in range(2):
        block = me if host == 0 else me + 1 - 2 * core

        def add(other, count):
            step = lax.rem(other - block + seg_len + seg_len // 2, seg_len) - seg_len // 2
            inside = (step >= -reach) & (step <= reach) & (other // 2 != me // 2)
            live = inside & (band_ref[host, jnp.clip(step + reach, 0, 2 * reach)] != 0)

            @pl.when(live)
            def _():
                list_ref[1 + count] = other
                list_ref[1 + n_list + 2 + count] = host

            return count + live.astype(jnp.int32)

        list_ref[0] = lax.fori_loop(0, seg_len, add, list_ref[0])

    for copy in copies:
        copy.wait()
    for host in range(2):
        for part in range(per_half):
            slot = host * CHUNKS + core * per_half + part
            block = vis[slot]
            extra = block[feat:feat + EXTRA].astype(jnp.float32)
            n_low = DEPTH - feat - EXTRA
            upper = jnp.concatenate([jnp.ones((3, width), jnp.float32), jnp.zeros((EXTRA - 3, width), jnp.float32)], axis=0)
            lower = jnp.concatenate([
                extra[SQUARE:SQUARE + 3], extra[CHARGE:CHARGE + 3], jnp.zeros((n_low - 6, width), jnp.float32)], axis=0)
            below = jnp.concatenate([upper, lower], axis=0).astype(jnp.bfloat16)
            full = jnp.concatenate([-2 * block[:feat], below], axis=0)
            host_ref[host, part * width:(part + 1) * width, :] = full.T
    host_charges(host_ref, charges, feat)

    def run(slot, host, gap):
        pair_task(vis.at[slot], host, gap, None, host_ref, charges, acc_ref, sum_ref)

    def masked(step, carry):
        host = step // per_half
        part = lax.rem(step, per_half)
        run(host * CHUNKS + core * per_half + part, host, -part * width)
        return carry

    def unmasked(step, carry):
        host = jnp.where(step < 2, step, lax.rem(step, 2))
        base = jnp.where(step < 2, host * CHUNKS + (1 - core) * per_half, (1 - host) * CHUNKS + (step // 2 - 1) * per_half)
        for part in range(per_half):
            run(base + part, host, None)
        return carry

    lax.fori_loop(0, CHUNKS, masked, 0)
    linked = band_ref[0, reach + 1 - 2 * core] != 0
    lax.fori_loop(0, jnp.where(linked, 6, 2), unmasked, 0)


def far_kernel(last, list_ref, vis_ref, host_ref, acc_old, sum_old, *refs):
    if last:
        (own_ref, partner_ref, out_ref, part_ref, energy_ref, vis, charges, acc_prev, sum_prev, sems, old_sems,
         acc_ref, sum_ref, x_buf, x_sems, out_sem) = refs
    else:
        acc_ref, sum_ref, vis, charges, acc_prev, sum_prev, sems, old_sems = refs
    feat = acc_ref.shape[1]
    width = vis.shape[3]
    n_list = (list_ref.shape[0] - 1) // 2
    count = list_ref[0]
    old = [pltpu.make_async_copy(acc_old, acc_prev, old_sems.at[0]), pltpu.make_async_copy(sum_old, sum_prev, old_sems.at[1])]

    def fetch(pair, slot):
        return [pltpu.make_async_copy(
            vis_ref.at[list_ref[1 + 2 * pair + u]], vis.at[slot, u, pl.ds(0, feat + EXTRA), :], sems.at[slot, u]) for u in range(2)]

    if last:
        per_half = acc_ref.shape[2] // width
        core = lax.rem(lax.axis_index('seg'), 2)
        for host, ref in enumerate((own_ref, partner_ref)):
            for part in range(per_half):
                old.append(pltpu.make_async_copy(
                    ref.at[core * per_half + part, pl.ds(0, feat), :], x_buf.at[host, :, pl.ds(part * width, width)], x_sems.at[host, part]))
    for copy in fetch(0, 0) + old:
        copy.start()
    low = lower_rows(feat, width)
    for slot in range(2):
        for u in range(2):
            vis[slot, u, feat + EXTRA:, :] = low
    clear_sums(acc_ref, sum_ref)
    host_charges(host_ref, charges, feat)

    def run(slot, u, task):
        pair_task(vis.at[slot, u], list_ref[1 + n_list + task], None, (task < count) if u else None, host_ref, charges, acc_ref, sum_ref)

    def two_tasks(pair, carry):
        slot = lax.rem(pair, 2)
        for copy in fetch(pair, slot):
            copy.wait()
        for copy in fetch(pair + 1, 1 - slot):
            copy.start()
        for u in range(2):
            run(slot, u, 2 * pair + u)
        return carry

    pairs = (count + 1) // 2
    lax.fori_loop(0, pairs, two_tasks, 0)
    for copy in fetch(pairs, lax.rem(pairs, 2)):
        copy.wait()

    for copy in old:
        copy.wait()
    if not last:
        def step(number, rows):
            (acc_ref, sum_ref)[number][rows] += (acc_prev, sum_prev)[number][rows]

        sweep(acc_ref, sum_ref, step)
        return
    half = acc_ref.shape[2]
    energy = jnp.zeros((8, 128), jnp.float32)
    place = pl.ds(pl.multiple_of(core * half, 128), half)
    store = pltpu.make_async_copy(acc_ref.at[0], out_ref.at[:, place], out_sem)
    for host, target in ((0, acc_ref.at[0]), (1, part_ref)):
        sums = sum_ref[host] + sum_prev[host]
        energy = energy + jnp.sum(sums.reshape(half // 8, 8, 128), axis=0)
        total = jnp.zeros((8, half), jnp.float32)
        for piece in pieces(sums):
            total = total + lax.dot_general(
                jnp.ones((8, 128), jnp.bfloat16), piece.astype(jnp.bfloat16), (((1,), (1,)), ((), ())), preferred_element_type=jnp.float32)
        pulled = acc_ref[host] + acc_prev[host]
        target[...] = (total[0:1] * x_buf[host].astype(jnp.float32) - pulled) * (1.0 / feat)
        if host == 0:
            store.start()
    energy_ref[...] = energy
    store.wait()


def join_kernel(mine_ref, other_ref, out_ref, bounce, sems):
    half = other_ref.shape[1]
    pieces_n = sems.shape[1]
    rows = other_ref.shape[0] // pieces_n
    core = lax.rem(lax.axis_index('seg'), 2)
    place = pl.ds(pl.multiple_of((1 - core) * half, 128), half)
    loads, stores = [], []
    for k in range(pieces_n):
        span = pl.ds(k * rows, rows)
        loads.append(pltpu.make_async_copy(other_ref.at[span], bounce.at[span], sems.at[0, k]))
        stores.append(pltpu.make_async_copy(bounce.at[span], out_ref.at[span, place], sems.at[1, k]))
        loads[-1].start()
    for load, store in zip(loads, stores):
        load.wait()
        store.start()
    for store in stores:
        store.wait()


def total_kernel(n, x_ref, out_ref, slots, send_sems, recv_sems):
    me = lax.axis_index('seg')
    barrier = pltpu.get_barrier_semaphore()
    for k in range(1, n):
        pl.semaphore_signal(barrier, inc=1, device_id={'seg': lax.rem(me + k, n)}, device_id_type=MESH)
    pl.semaphore_wait(barrier, n - 1)
    sends = []
    for k in range(1, n):
        sends.append(pltpu.make_async_remote_copy(
            src_ref=x_ref, dst_ref=slots.at[me], send_sem=send_sems.at[k], recv_sem=recv_sems.at[me],
            device_id={'seg': lax.rem(me + k, n)}, device_id_type=MESH))
        sends[-1].start()
    slots[me] = x_ref[...]
    for k in range(1, n):
        owner = lax.rem(me + k, n)
        pltpu.make_async_remote_copy(
            src_ref=x_ref, dst_ref=slots.at[owner], send_sem=send_sems.at[k], recv_sem=recv_sems.at[owner],
            device_id={'seg': owner}, device_id_type=MESH).wait_recv()
    for send in sends:
        send.wait_send()
    total = slots[0]
    for k in range(1, n):
        total = total + slots[k]
    out_ref[...] = total


def solution(mesh):
    seg_len = mesh.shape['seg']
    swap = [(dev, dev ^ 1) for dev in range(seg_len)]
    any_space = pl.BlockSpec(memory_space=pl.ANY)
    vmem = pl.BlockSpec(memory_space=pltpu.VMEM)
    smem = pl.BlockSpec(memory_space=pltpu.SMEM)

    def device_fn(positions, charges, pair_band):
        n_rows, feat = positions.shape
        reach = (pair_band.shape[1] - 1) // 2
        half = n_rows // 2
        width = n_rows // CHUNKS
        shape = jax.ShapeDtypeStruct
        big = pltpu.CompilerParams(vmem_limit_bytes=60 * 2 ** 20)
        packed = (feat + EXTRA, width)

        x_t = positions.T
        charge_row = charges[None, :]
        first_part = pl.pallas_call(
            functools.partial(pack_kernel, (0,)),
            grid=(1,),
            out_shape=shape(packed, jnp.bfloat16),
            in_specs=[pl.BlockSpec((feat, width), lambda i: (0, 0)), pl.BlockSpec((1, width), lambda i: (0, 0))],
            out_specs=pl.BlockSpec(packed, lambda i: (0, 0)),
            name='pack_first',
        )(x_t, charge_row)
        *parts, own = pl.pallas_call(
            functools.partial(pack_kernel, tuple(range(CHUNKS))),
            out_shape=[shape(packed, jnp.bfloat16)] * (CHUNKS - 1) + [shape((CHUNKS,) + packed, jnp.bfloat16)],
            in_specs=[vmem, vmem],
            out_specs=[vmem] * CHUNKS,
            compiler_params=big,
            name='pack',
        )(x_t, charge_row)
        parts = [first_part] + parts
        gathered = [lax.all_gather(part, 'seg') for part in parts]
        partner = lax.ppermute(own, 'seg', swap)
        bands = jnp.concatenate([pair_band, lax.ppermute(pair_band, 'seg', swap)])

        acc_shape = shape((2, feat, half), jnp.float32)
        sum_shape = shape((2, half, 128), jnp.float32)
        host_shape = shape((2, half, DEPTH), jnp.bfloat16)
        n_list = 2 * seg_len + 2
        pair_flops = 4 * half * width * DEPTH
        tasks, host, acc, sums = pl.pallas_call(
            functools.partial(near_kernel, seg_len, reach),
            out_shape=[shape((1 + 2 * n_list,), jnp.int32), host_shape, acc_shape, sum_shape],
            in_specs=[smem, any_space, any_space],
            out_specs=[smem, vmem, vmem, vmem],
            scratch_shapes=[
                pltpu.VMEM((2 * CHUNKS, DEPTH, width), jnp.bfloat16),
                pltpu.VMEM((2, half, 128), jnp.float32),
                pltpu.SemaphoreType.DMA((2 * CHUNKS,)),
            ],
            compiler_params=big,
            cost_estimate=pl.CostEstimate(flops=16 * pair_flops, bytes_accessed=2 ** 24, transcendentals=16 * half * width),
            name='near_pairs',
        )(bands, own, partner)
        for chunk, block in enumerate(gathered):
            last = chunk == CHUNKS - 1
            scratch = [
                pltpu.VMEM((2, 2, DEPTH, width), jnp.bfloat16),
                pltpu.VMEM((2, half, 128), jnp.float32),
                pltpu.VMEM(acc_shape.shape, jnp.float32),
                pltpu.VMEM(sum_shape.shape, jnp.float32),
                pltpu.SemaphoreType.DMA((2, 2)),
                pltpu.SemaphoreType.DMA((2,)),
            ]
            if last:
                scratch += [
                    pltpu.VMEM(acc_shape.shape, jnp.float32),
                    pltpu.VMEM(sum_shape.shape, jnp.float32),
                    pltpu.VMEM(acc_shape.shape, jnp.bfloat16),
                    pltpu.SemaphoreType.DMA((2, CHUNKS // 2)),
                    pltpu.SemaphoreType.DMA,
                ]
                out_shape = [shape((feat, n_rows), jnp.float32), shape((feat, half), jnp.float32), shape((8, 128), jnp.float32)]
            else:
                out_shape = [acc_shape, sum_shape]
            acc, sums, *energy_part = pl.pallas_call(
                functools.partial(far_kernel, last),
                out_shape=out_shape,
                in_specs=[smem, any_space, vmem, any_space, any_space] + [any_space] * (2 if last else 0),
                out_specs=[any_space if last else vmem] + [vmem] * (len(out_shape) - 1),
                scratch_shapes=scratch,
                compiler_params=big,
                cost_estimate=pl.CostEstimate(flops=20 * pair_flops, bytes_accessed=2 ** 25, transcendentals=20 * half * width),
                name='last_pairs' if last else 'far_pairs',
            )(tasks, block, host, acc, sums, *((own, partner) if last else ()))

        other = lax.ppermute(sums, 'seg', swap)
        energy_all = pl.pallas_call(
            functools.partial(total_kernel, seg_len),
            out_shape=shape((8, 128), jnp.float32),
            in_specs=[vmem],
            out_specs=vmem,
            scratch_shapes=[
                pltpu.VMEM((seg_len, 8, 128), jnp.float32),
                pltpu.SemaphoreType.DMA((seg_len,)),
                pltpu.SemaphoreType.DMA((seg_len,)),
            ],
            compiler_params=pltpu.CompilerParams(collective_id=0, has_side_effects=True),
            name='energy_total',
        )(energy_part[0])
        energy = 0.5 * jnp.sum(energy_all)

        forces = pl.pallas_call(
            join_kernel,
            out_shape=shape((feat, n_rows), jnp.float32),
            in_specs=[any_space, any_space],
            out_specs=any_space,
            scratch_shapes=[pltpu.VMEM((feat, half), jnp.float32), pltpu.SemaphoreType.DMA((2, 4))],
            input_output_aliases={0: 0},
            name='join_halves',
        )(acc, other)
        return forces.T, energy.reshape(1)

    row_spec = P(('sys', 'seg'), None)
    vec_spec = P(('sys', 'seg'))
    return jax.shard_map(device_fn, mesh=mesh, in_specs=(row_spec, vec_spec, row_spec), out_specs=(row_spec, P('sys')), check_vma=False)
```

```python
import functools
import math

import jax
import jax.numpy as jnp
from jax import lax
from jax.experimental import pallas as pl
from jax.experimental.pallas import tpu as pltpu
from jax.sharding import PartitionSpec as P

CHUNKS = 6
GATHERS = 3
JOINED = CHUNKS // GATHERS
TILE = 256
EXTRA = 8
DEPTH = 384
MESH = pl.DeviceIdType.MESH

SQUARE, CHARGE, HOST_CHARGE = 0, 3, 11


def pieces(values):
    high = values.astype(jnp.bfloat16).astype(jnp.float32)
    rest = values - high
    mid = rest.astype(jnp.bfloat16).astype(jnp.float32)
    return [high, mid, rest - mid]


def pack_kernel(chunks, x_ref, q_ref, *out_refs):
    feat = x_ref.shape[0]
    width = out_refs[-1].shape[-1]
    for chunk in chunks:
        cols = slice(chunk * width, (chunk + 1) * width)
        x = x_ref[:, cols]
        xf = x.astype(jnp.float32)
        square = jnp.minimum(jnp.sum(xf * xf, axis=0, keepdims=True), 3.0e38)
        extra = jnp.concatenate(pieces(square) + pieces(q_ref[:, cols]) + [jnp.zeros((EXTRA - 6, width), jnp.float32)], axis=0)
        extra = extra.astype(jnp.bfloat16)
        targets = out_refs if len(chunks) == 1 else [out_refs[-1].at[chunk]]
        if len(chunks) > 1 and chunk >= JOINED:
            targets.append(out_refs[chunk // JOINED - 1].at[:, pl.ds(chunk % JOINED * width, width)])
        for ref in targets:
            ref[:feat, :] = x
            ref[feat:, :] = extra


def lower_rows(feat, width):
    n_low = DEPTH - feat - EXTRA
    row = lax.broadcasted_iota(jnp.int32, (n_low, width), 0)
    return jnp.where(row < 3, 1.0, 0.0).astype(jnp.bfloat16)


def pair_task(vis_ref, host, gap, host_ref, charge_ref, acc_ref, sum_ref):
    feat, half = acc_ref.shape[1:]
    width = vis_ref.shape[1]
    scale = -math.log2(math.e) * 0.5 / feat
    extra = vis_ref[feat:feat + EXTRA, :].astype(jnp.float32)
    charge_j = extra[CHARGE:CHARGE + 1] + extra[CHARGE + 1:CHARGE + 2] + extra[CHARGE + 2:CHARGE + 3]

    def span(tile):
        return slice(tile * TILE, (tile + 1) * TILE)

    def distance(tile):
        return jnp.dot(host_ref[host, span(tile), :], vis_ref[...], preferred_element_type=jnp.float32)

    def pull(weights, tile):
        acc_ref[host, :, span(tile)] += lax.dot_general(
            vis_ref[:feat, :], weights, (((1,), (1,)), ((), ())), preferred_element_type=jnp.float32)

    n_tiles = half // TILE
    ahead = distance(0)
    behind = None
    for tile in range(n_tiles):
        charge_i = jnp.concatenate([charge_ref[host, span(tile), :]] * (width // 128), axis=1)
        weights = jnp.exp2(jnp.maximum(ahead, 0.0) * scale) * charge_i * charge_j
        if gap is not None:
            row = lax.broadcasted_iota(jnp.int32, weights.shape, 0)
            col = lax.broadcasted_iota(jnp.int32, weights.shape, 1)
            weights = jnp.where(col - row == gap + tile * TILE, 0.0, weights)
        part = weights[:, :128]
        for group in range(1, width // 128):
            part = part + weights[:, group * 128:(group + 1) * 128]
        sum_ref[host, span(tile), :] += part
        if tile + 1 < n_tiles:
            ahead = distance(tile + 1)
        if behind is not None:
            pull(behind, tile - 1)
        behind = weights.astype(jnp.bfloat16)
    pull(behind, n_tiles - 1)


def sweep(acc_ref, sum_ref, step):
    for number, ref, rows in ((0, acc_ref, 64), (1, sum_ref, 512)):
        def one(k, carry):
            step(number, (slice(None), pl.ds(pl.multiple_of(k * rows, 8), rows), slice(None)))
            return carry

        lax.fori_loop(0, ref.shape[1] // rows, one, 0)


def clear_sums(acc_ref, sum_ref):
    refs = (acc_ref, sum_ref)

    def step(number, rows):
        refs[number][rows] = jnp.zeros_like(refs[number][rows])

    sweep(acc_ref, sum_ref, step)


def host_charges(host_ref, charge_ref, feat):
    base = DEPTH - 128
    row = lax.broadcasted_iota(jnp.int32, (128, 128), 0) + base - feat - HOST_CHARGE
    pick = jnp.where((row >= 0) & (row < 3), 1.0, 0.0).astype(jnp.bfloat16)
    for host in range(2):
        charge_ref[host] = jnp.dot(host_ref[host, :, base:], pick, preferred_element_type=jnp.float32)


def near_kernel(seg_len, reach, band_ref, own_ref, partner_ref, list_ref, host_ref, acc_ref, sum_ref, vis, charges, sems):
    feat = own_ref.shape[1] - EXTRA
    width = own_ref.shape[2]
    half = CHUNKS * width // 2
    per_half = CHUNKS // 2
    me = lax.axis_index('seg')
    core = lax.rem(me, 2)
    copies = []
    for side, ref in enumerate((own_ref, partner_ref)):
        for chunk in range(CHUNKS):
            slot = side * CHUNKS + chunk
            copies.append(pltpu.make_async_copy(ref.at[chunk], vis.at[slot, pl.ds(0, feat + EXTRA), :], sems.at[slot]))
            copies[-1].start()
    low = lower_rows(feat, width)
    for slot in range(2 * CHUNKS):
        vis[slot, feat + EXTRA:, :] = low
    clear_sums(acc_ref, sum_ref)

    n_list = 2 * seg_len
    list_ref[0] = 0

    def clear(i, carry):
        list_ref[i] = 0
        return carry

    lax.fori_loop(0, list_ref.shape[0], clear, 0)
    for host in range(2):
        block = me if host == 0 else me + 1 - 2 * core

        def add(other, count):
            step = lax.rem(other - block + seg_len + seg_len // 2, seg_len) - seg_len // 2
            inside = (step >= -reach) & (step <= reach) & (other // 2 != me // 2)
            live = inside & (band_ref[host, jnp.clip(step + reach, 0, 2 * reach)] != 0)

            @pl.when(live)
            def _():
                list_ref[1 + count] = other
                list_ref[1 + n_list + 2 + count] = host

            return count + live.astype(jnp.int32)

        list_ref[0] = lax.fori_loop(0, seg_len, add, list_ref[0])

    for copy in copies:
        copy.wait()
    for host in range(2):
        for part in range(per_half):
            slot = host * CHUNKS + core * per_half + part
            block = vis[slot]
            extra = block[feat:feat + EXTRA].astype(jnp.float32)
            n_low = DEPTH - feat - EXTRA
            upper = jnp.concatenate([jnp.ones((3, width), jnp.float32), jnp.zeros((EXTRA - 3, width), jnp.float32)], axis=0)
            lower = jnp.concatenate([
                extra[SQUARE:SQUARE + 3], extra[CHARGE:CHARGE + 3], jnp.zeros((n_low - 6, width), jnp.float32)], axis=0)
            below = jnp.concatenate([upper, lower], axis=0).astype(jnp.bfloat16)
            full = jnp.concatenate([-2 * block[:feat], below], axis=0)
            host_ref[host, part * width:(part + 1) * width, :] = full.T
    host_charges(host_ref, charges, feat)

    def run(slot, host, gap):
        pair_task(vis.at[slot], host, gap, host_ref, charges, acc_ref, sum_ref)

    def masked(step, carry):
        host = step // per_half
        part = lax.rem(step, per_half)
        run(host * CHUNKS + core * per_half + part, host, -part * width)
        return carry

    def unmasked(step, carry):
        cross = step - CHUNKS
        host = jnp.where(step < CHUNKS, step // per_half, cross // CHUNKS)
        base = jnp.where(step < CHUNKS, host * CHUNKS + (1 - core) * per_half + lax.rem(step, per_half), (1 - host) * CHUNKS + lax.rem(step, CHUNKS))
        run(base, host, None)
        return carry

    lax.fori_loop(0, CHUNKS, masked, 0)
    linked = band_ref[0, reach + 1 - 2 * core] != 0
    lax.fori_loop(0, jnp.where(linked, 3 * CHUNKS, CHUNKS), unmasked, 0)


def far_kernel(last, list_ref, vis_ref, host_ref, acc_old, sum_old, *refs):
    if last:
        (own_ref, partner_ref, out_ref, part_ref, energy_ref, vis, charges, acc_prev, sum_prev, sems, old_sems,
         acc_ref, sum_ref, x_buf, x_sems, out_sem) = refs
    else:
        acc_ref, sum_ref, vis, charges, acc_prev, sum_prev, sems, old_sems = refs
    feat = acc_ref.shape[1]
    width = vis.shape[2] // JOINED
    n_list = (list_ref.shape[0] - 1) // 2
    count = list_ref[0]
    old = [pltpu.make_async_copy(acc_old, acc_prev, old_sems.at[0]), pltpu.make_async_copy(sum_old, sum_prev, old_sems.at[1])]

    def fetch(task, slot):
        return pltpu.make_async_copy(vis_ref.at[list_ref[1 + task]], vis.at[slot, pl.ds(0, feat + EXTRA), :], sems.at[slot])

    if last:
        per_half = acc_ref.shape[2] // width
        core = lax.rem(lax.axis_index('seg'), 2)
        for host, ref in enumerate((own_ref, partner_ref)):
            for part in range(per_half):
                old.append(pltpu.make_async_copy(
                    ref.at[core * per_half + part, pl.ds(0, feat), :], x_buf.at[host, :, pl.ds(part * width, width)], x_sems.at[host, part]))
    for copy in [fetch(0, 0)] + old:
        copy.start()
    low = lower_rows(feat, width * JOINED)
    for slot in range(2):
        vis[slot, feat + EXTRA:, :] = low
    clear_sums(acc_ref, sum_ref)
    host_charges(host_ref, charges, feat)

    def one_task(task, carry):
        slot = lax.rem(task, 2)
        fetch(task, slot).wait()
        fetch(task + 1, 1 - slot).start()
        for part in range(JOINED):
            pair_task(
                vis.at[slot, :, pl.ds(part * width, width)], list_ref[1 + n_list + task], None, host_ref, charges, acc_ref, sum_ref)
        return carry

    lax.fori_loop(0, count, one_task, 0)
    fetch(count, lax.rem(count, 2)).wait()
    for copy in old:
        copy.wait()
    if not last:
        def step(number, rows):
            (acc_ref, sum_ref)[number][rows] += (acc_prev, sum_prev)[number][rows]

        sweep(acc_ref, sum_ref, step)
        return
    half = acc_ref.shape[2]
    energy = jnp.zeros((8, 128), jnp.float32)
    place = pl.ds(pl.multiple_of(core * half, 128), half)
    store = pltpu.make_async_copy(acc_ref.at[0], out_ref.at[:, place], out_sem)
    for host, target in ((0, acc_ref.at[0]), (1, part_ref)):
        sums = sum_ref[host] + sum_prev[host]
        energy = energy + jnp.sum(sums.reshape(half // 8, 8, 128), axis=0)
        total = jnp.zeros((8, half), jnp.float32)
        for piece in pieces(sums):
            total = total + lax.dot_general(
                jnp.ones((8, 128), jnp.bfloat16), piece.astype(jnp.bfloat16), (((1,), (1,)), ((), ())), preferred_element_type=jnp.float32)
        pulled = acc_ref[host] + acc_prev[host]
        target[...] = (total[0:1] * x_buf[host].astype(jnp.float32) - pulled) * (1.0 / feat)
        if host == 0:
            store.start()
    energy_ref[...] = energy
    store.wait()


def join_kernel(mine_ref, other_ref, out_ref, bounce, sems):
    half = other_ref.shape[1]
    pieces_n = sems.shape[1]
    rows = other_ref.shape[0] // pieces_n
    core = lax.rem(lax.axis_index('seg'), 2)
    place = pl.ds(pl.multiple_of((1 - core) * half, 128), half)
    loads, stores = [], []
    for k in range(pieces_n):
        span = pl.ds(k * rows, rows)
        loads.append(pltpu.make_async_copy(other_ref.at[span], bounce.at[span], sems.at[0, k]))
        stores.append(pltpu.make_async_copy(bounce.at[span], out_ref.at[span, place], sems.at[1, k]))
        loads[-1].start()
    for load, store in zip(loads, stores):
        load.wait()
        store.start()
    for store in stores:
        store.wait()


def total_kernel(n, x_ref, out_ref, slots, send_sems, recv_sems):
    me = lax.axis_index('seg')
    barrier = pltpu.get_barrier_semaphore()
    for k in range(1, n):
        pl.semaphore_signal(barrier, inc=1, device_id={'seg': lax.rem(me + k, n)}, device_id_type=MESH)
    pl.semaphore_wait(barrier, n - 1)
    sends = []
    for k in range(1, n):
        sends.append(pltpu.make_async_remote_copy(
            src_ref=x_ref, dst_ref=slots.at[me], send_sem=send_sems.at[k], recv_sem=recv_sems.at[me],
            device_id={'seg': lax.rem(me + k, n)}, device_id_type=MESH))
        sends[-1].start()
    slots[me] = x_ref[...]
    for k in range(1, n):
        owner = lax.rem(me + k, n)
        pltpu.make_async_remote_copy(
            src_ref=x_ref, dst_ref=slots.at[owner], send_sem=send_sems.at[k], recv_sem=recv_sems.at[owner],
            device_id={'seg': owner}, device_id_type=MESH).wait_recv()
    for send in sends:
        send.wait_send()
    total = slots[0]
    for k in range(1, n):
        total = total + slots[k]
    out_ref[...] = total


def solution(mesh):
    seg_len = mesh.shape['seg']
    swap = [(dev, dev ^ 1) for dev in range(seg_len)]
    any_space = pl.BlockSpec(memory_space=pl.ANY)
    vmem = pl.BlockSpec(memory_space=pltpu.VMEM)
    smem = pl.BlockSpec(memory_space=pltpu.SMEM)

    def device_fn(positions, charges, pair_band):
        n_rows, feat = positions.shape
        reach = (pair_band.shape[1] - 1) // 2
        half = n_rows // 2
        width = n_rows // CHUNKS
        shape = jax.ShapeDtypeStruct
        big = pltpu.CompilerParams(vmem_limit_bytes=60 * 2 ** 20)
        packed = (feat + EXTRA, width)
        sent = (feat + EXTRA, width * JOINED)

        x_t = positions.T
        charge_row = charges[None, :]
        first_part = pl.pallas_call(
            functools.partial(pack_kernel, (0,)),
            grid=(1,),
            out_shape=shape(sent, jnp.bfloat16),
            in_specs=[pl.BlockSpec((feat, sent[1]), lambda i: (0, 0)), pl.BlockSpec((1, sent[1]), lambda i: (0, 0))],
            out_specs=pl.BlockSpec(sent, lambda i: (0, 0)),
            name='pack_first',
        )(x_t, charge_row)
        *parts, own = pl.pallas_call(
            functools.partial(pack_kernel, tuple(range(CHUNKS))),
            out_shape=[shape(sent, jnp.bfloat16)] * (GATHERS - 1) + [shape((CHUNKS,) + packed, jnp.bfloat16)],
            in_specs=[vmem, vmem],
            out_specs=[vmem] * GATHERS,
            compiler_params=big,
            name='pack',
        )(x_t, charge_row)
        parts = [first_part] + parts
        gathered = [lax.all_gather(part, 'seg') for part in parts]
        partner = lax.ppermute(own, 'seg', swap)
        bands = jnp.concatenate([pair_band, lax.ppermute(pair_band, 'seg', swap)])

        acc_shape = shape((2, feat, half), jnp.float32)
        sum_shape = shape((2, half, 128), jnp.float32)
        host_shape = shape((2, half, DEPTH), jnp.bfloat16)
        n_list = 2 * seg_len + 2
        pair_flops = 4 * half * width * DEPTH
        tasks, host, acc, sums = pl.pallas_call(
            functools.partial(near_kernel, seg_len, reach),
            out_shape=[shape((1 + 2 * n_list,), jnp.int32), host_shape, acc_shape, sum_shape],
            in_specs=[smem, any_space, any_space],
            out_specs=[smem, vmem, vmem, vmem],
            scratch_shapes=[
                pltpu.VMEM((2 * CHUNKS, DEPTH, width), jnp.bfloat16),
                pltpu.VMEM((2, half, 128), jnp.float32),
                pltpu.SemaphoreType.DMA((2 * CHUNKS,)),
            ],
            compiler_params=big,
            cost_estimate=pl.CostEstimate(flops=16 * pair_flops, bytes_accessed=2 ** 24, transcendentals=16 * half * width),
            name='near_pairs',
        )(bands, own, partner)
        for chunk, block in enumerate(gathered):
            last = chunk == GATHERS - 1
            scratch = [
                pltpu.VMEM((2, DEPTH, sent[1]), jnp.bfloat16),
                pltpu.VMEM((2, half, 128), jnp.float32),
                pltpu.VMEM(acc_shape.shape, jnp.float32),
                pltpu.VMEM(sum_shape.shape, jnp.float32),
                pltpu.SemaphoreType.DMA((2,)),
                pltpu.SemaphoreType.DMA((2,)),
            ]
            if last:
                scratch += [
                    pltpu.VMEM(acc_shape.shape, jnp.float32),
                    pltpu.VMEM(sum_shape.shape, jnp.float32),
                    pltpu.VMEM(acc_shape.shape, jnp.bfloat16),
                    pltpu.SemaphoreType.DMA((2, CHUNKS // 2)),
                    pltpu.SemaphoreType.DMA,
                ]
                out_shape = [shape((feat, n_rows), jnp.float32), shape((feat, half), jnp.float32), shape((8, 128), jnp.float32)]
            else:
                out_shape = [acc_shape, sum_shape]
            acc, sums, *energy_part = pl.pallas_call(
                functools.partial(far_kernel, last),
                out_shape=out_shape,
                in_specs=[smem, any_space, vmem, any_space, any_space] + [any_space] * (2 if last else 0),
                out_specs=[any_space if last else vmem] + [vmem] * (len(out_shape) - 1),
                scratch_shapes=scratch,
                compiler_params=big,
                cost_estimate=pl.CostEstimate(flops=40 * pair_flops, bytes_accessed=2 ** 25, transcendentals=40 * half * width),
                name='last_pairs' if last else 'far_pairs',
            )(tasks, block, host, acc, sums, *((own, partner) if last else ()))

        other = lax.ppermute(sums, 'seg', swap)
        energy_all = pl.pallas_call(
            functools.partial(total_kernel, seg_len),
            out_shape=shape((8, 128), jnp.float32),
            in_specs=[vmem],
            out_specs=vmem,
            scratch_shapes=[
                pltpu.VMEM((seg_len, 8, 128), jnp.float32),
                pltpu.SemaphoreType.DMA((seg_len,)),
                pltpu.SemaphoreType.DMA((seg_len,)),
            ],
            compiler_params=pltpu.CompilerParams(collective_id=0, has_side_effects=True),
            name='energy_total',
        )(energy_part[0])
        energy = 0.5 * jnp.sum(energy_all)

        forces = pl.pallas_call(
            join_kernel,
            out_shape=shape((feat, n_rows), jnp.float32),
            in_specs=[any_space, any_space],
            out_specs=any_space,
            scratch_shapes=[pltpu.VMEM((feat, half), jnp.float32), pltpu.SemaphoreType.DMA((2, 4))],
            input_output_aliases={0: 0},
            name='join_halves',
        )(acc, other)
        return forces.T, energy.reshape(1)

    row_spec = P(('sys', 'seg'), None)
    vec_spec = P(('sys', 'seg'))
    return jax.shard_map(device_fn, mesh=mesh, in_specs=(row_spec, vec_spec, row_spec), out_specs=(row_spec, P('sys')), check_vma=False)
```
